32 devices in a mesh: frame: 4 (over z), row: 8 (over y, x, core).
Axes of the slice: x: 2, y: 2, z: 4, core: 2. Of those that a mesh axis runs over, the one named last changes fastest.
Arguments:
- fine: bfloat16 [8, 320, 32, 128], P('frame', None, 'row'), may hold values from -6 to 6
- coarse: bfloat16 [4, 64, 1280], P(None, 'row', 'frame'), may hold values from -6 to 6
- w_qkv: bfloat16 [3, 1280, 1280], P(None, None, 'frame'), may hold values from -0.15625 to 0.15625
- w_out: bfloat16 [1280, 1280], P('frame'), may hold values from -0.15625 to 0.15625
- w_up: bfloat16 [1280, 320], P('frame'), may hold values from -0.15625 to 0.15625
- gain_one: float32 [320], replicated, may hold values from 0.1 to 1.9
- conv_space: bfloat16 [3, 3, 320, 320], replicated, may hold values from -0.109375 to 0.109375
- gain_two: float32 [320], replicated, may hold values from 0.1 to 1.9
- conv_time: bfloat16 [3, 320, 320], replicated, may hold values from -0.1875 to 0.1875
Outputs:
- result: bfloat16 [8, 320, 32, 128], P('frame', None, 'row')
The draws below stay inside these ranges and needn't reach their ends.
All inputs are finite; a program needn't handle non-finite values.
Results may differ from the reference program's by a relative error of at most 0.013.
Values may be sent and summed in bfloat16 or wider, within the bound.
A program may use at most 64 MiB of HBM per device.

```python
import math
import jax
import jax.numpy as jnp
from jax import lax

C = 320
CC = 1280
HEADS = 16
HD = 80
W = 128
CF = 4
FRAMES = 8
ROWS = 32
CH = 4
CW = 16
CP = 64


def shard_levels(own_key, dims, shards, least, top_value):
    def one(dim, parts):
        draws = jax.random.uniform(jax.random.fold_in(jax.random.fold_in(own_key, 6), dim), (parts,), jnp.float32, least / len(shards), top_value / len(shards))
        return jnp.repeat(jnp.exp(draws), dims[dim] // parts).reshape((-1,) + (1,) * (len(dims) - dim - 1))

    loudness = one(*shards[0])
    for cut in shards[1:]:
        loudness = loudness * one(*cut)
    return loudness


def gaussian(rng, shape, scale, most, split=(), held_as=jnp.bfloat16):
    result = scale * jax.random.normal(rng, shape, jnp.float32)
    if split:
        result = result * shard_levels(rng, shape, split, -0.22, 0.18)
    return jnp.clip(result, -most, most).astype(held_as)


def setup_inputs(seed: int = 0) -> dict:
    seeds = jax.random.split(jax.random.key(seed), 10)
    return {
        "fine": gaussian(seeds[0], (FRAMES, C, ROWS, W), 1.0, 6.0, ((0, 4), (2, 8))),
        "coarse": gaussian(seeds[1], (CF, CP, CC), 1.0, 6.0, ((1, 8), (2, 4))),
        "w_qkv": gaussian(seeds[2], (3, CC, CC), CC ** -0.5, 0.15625, ((2, 4),)),
        "w_out": gaussian(seeds[3], (CC, CC), CC ** -0.5, 0.15625, ((0, 4),)),
        "w_up": gaussian(seeds[4], (CC, C), CC ** -0.5, 0.15625, ((0, 4),)),
        "gain_one": jnp.clip(1.0 + 0.18 * jax.random.normal(seeds[5], (C,), jnp.float32), 0.1, 1.9),
        "conv_space": gaussian(seeds[6], (3, 3, C, C), (9 * C) ** -0.5, 0.109375),
        "gain_two": jnp.clip(1.0 + 0.18 * jax.random.normal(seeds[7], (C,), jnp.float32), 0.1, 1.9),
        "conv_time": gaussian(seeds[8], (3, C, C), (3 * C) ** -0.5, 0.1875),
    }


def norm_silu(values, gain):
    square = lax.optimization_barrier(jnp.mean(values * values, axis=-3, keepdims=True))
    scaled = values * lax.rsqrt(square + 1e-06) * gain[:, None, None]
    return jax.nn.silu(scaled).astype(jnp.bfloat16)

def reference(fine, coarse, w_qkv, w_out, w_up, gain_one, conv_space, gain_two, conv_time):
    qkv = jnp.einsum('fpc,icd->ifpd', coarse.astype(jnp.float32), w_qkv.astype(jnp.float32)).astype(jnp.bfloat16)
    query = qkv[0].reshape(CF, CP, HEADS, HD).astype(jnp.float32)
    keys = qkv[1].reshape(CF, CP, HEADS, HD).astype(jnp.float32)
    values = qkv[2].reshape(CF, CP, HEADS, HD).astype(jnp.float32)
    scores = jnp.einsum('fphd,gphd->phfg', query, keys) / math.sqrt(HD)
    probs = jax.nn.softmax(scores, axis=-1).astype(jnp.bfloat16)
    attn = jnp.einsum('phfg,gphd->fphd', probs.astype(jnp.float32), values).astype(jnp.bfloat16).reshape(CF * CP, CC)
    projected = jnp.dot(attn, w_out, preferred_element_type=jnp.float32)
    coarse_out = (coarse.reshape(CF * CP, CC).astype(jnp.float32) + projected).astype(jnp.bfloat16)
    upward = jnp.dot(coarse_out, w_up, preferred_element_type=jnp.float32).astype(jnp.bfloat16)
    upward = upward.reshape(CF, CH, CW, C)

    def first_half(index):
        coarse_frame = (index * CF // FRAMES).astype(jnp.int32)
        cells = lax.dynamic_index_in_dim(upward, coarse_frame, 0, keepdims=False)
        spread = jnp.repeat(jnp.repeat(cells, 8, axis=0), 8, axis=1)
        spread = jnp.transpose(spread, (2, 0, 1)).astype(jnp.float32)
        frame_in = lax.dynamic_index_in_dim(fine, index, 0, keepdims=False).astype(jnp.float32)
        merged = (frame_in + spread).astype(jnp.bfloat16)
        first = norm_silu(merged.astype(jnp.float32), gain_one)
        padded = jnp.pad(first.astype(jnp.float32), ((0, 0), (1, 1), (1, 1)))
        spatial = jnp.zeros((C, ROWS, W), jnp.float32)
        for offset_y in range(3):
            for offset_x in range(3):
                window = padded[:, offset_y:offset_y + ROWS, offset_x:offset_x + W]
                spatial = spatial + jnp.einsum('crw,cd->drw', window, conv_space[offset_y, offset_x].astype(jnp.float32))
        return (merged, norm_silu(spatial, gain_two))
    merged_all, second_all = lax.map(first_half, jnp.arange(FRAMES, dtype=jnp.int32))
    padded_time = jnp.pad(second_all, ((1, 1), (0, 0), (0, 0), (0, 0)))

    def second_half(index):
        window = lax.dynamic_slice_in_dim(padded_time, index, 3, 0)
        temporal = jnp.zeros((C, ROWS, W), jnp.float32)
        for offset in range(3):
            temporal = temporal + jnp.einsum('crw,cd->drw', window[offset].astype(jnp.float32), conv_time[offset].astype(jnp.float32))
        merged = lax.dynamic_index_in_dim(merged_all, index, 0, keepdims=False).astype(jnp.float32)
        return (merged + temporal).astype(jnp.bfloat16)
    return lax.map(second_half, jnp.arange(FRAMES, dtype=jnp.int32))
```

```python
import functools
import math

import jax
import jax.numpy as jnp
from jax import lax
from jax.experimental import pallas as pl
from jax.experimental.pallas import tpu as pltpu
from jax.sharding import PartitionSpec as P

HD = 80
UPSAMPLE = 8
MESH = pl.DeviceIdType.MESH
BF = jnp.bfloat16
F32 = jnp.float32


def dot(a, b):
    return jnp.dot(a, b, preferred_element_type=F32)


def dot_t(a, b):
    return lax.dot_general(a, b, (((0,), (0,)), ((), ())), preferred_element_type=F32)


def norm_silu(v, half_gain):
    scale = lax.rsqrt(jnp.mean(v * v, axis=0, keepdims=True) + 1e-06)
    half = v * scale * half_gain
    return half + half * jnp.tanh(half)


def kernel(
    nf, nr, cf_count, p_dev, rows,
    fine_ref, coarse_ref, w_qkv_ref, w_out_ref, w_up_ref, gain_one_ref, conv_s_ref, gain_two_ref, conv_t_ref,
    out_ref,
    cv, g1, g2, ff, wq, wo, wu, cs, ct, cst, ctt, fb, mg, cg, rs_send, rs_recv, up_send, up_recv, ub, x3, n2,
    half_one, half_two, o32, ov,
    load_sem, halo_send, halo_recv, g_send, g_recv, r_send, r_recv, u_send, u_recv, b_send, b_recv, out_sem,
):
    f_dev, flat, width = fine_ref.shape
    chans = flat // rows
    cells, c_dev = coarse_ref.shape
    frames_ext = f_dev + 2
    rows_ext = rows + 2
    group = (width // UPSAMPLE) // p_dev
    n_groups = nr // group
    heads = c_dev // HD
    span = group * p_dev
    total_frames = nf * f_dev
    me_f = lax.axis_index("frame")
    me_r = lax.axis_index("row")
    my_group = me_r // group
    k_me = me_r % group
    base = my_group * group
    first = k_me == 0
    last = k_me == group - 1
    has_above = first & (my_group > 0)
    has_below = last & (my_group < n_groups - 1)

    def dev(f, r):
        return {"frame": f, "row": r}

    barrier = pltpu.get_barrier_semaphore()
    for step_f in range(nf):
        for step_k in range(group):
            if step_f or step_k:
                peer = dev((me_f + step_f) % nf, base + (k_me + step_k) % group)
                pl.semaphore_signal(barrier, inc=1, device_id=peer, device_id_type=MESH)
    expected = jnp.int32(nf * group - 1)
    for ok, peer in ((has_above, me_r - 1), (has_below, me_r + 1)):
        expected = expected + ok.astype(jnp.int32)

        @pl.when(ok)
        def _(peer=peer):
            pl.semaphore_signal(barrier, inc=1, device_id=dev(me_f, peer), device_id_type=MESH)

    parts = {
        "coarse": (coarse_ref, cv),
        "fine": (fine_ref, ff),
        "gain_one": (gain_one_ref, g1),
        "gain_two": (gain_two_ref, g2),
        "qkv": (w_qkv_ref, wq),
        "out": (w_out_ref, wo),
        "space0": (conv_s_ref.at[0], cs.at[0]),
        "up": (w_up_ref, wu),
        "space1": (conv_s_ref.at[1], cs.at[1]),
        "space2": (conv_s_ref.at[2], cs.at[2]),
        "time": (conv_t_ref, ct),
    }
    loads = {
        name: pltpu.make_async_copy(src, dst, load_sem.at[n])
        for n, (name, (src, dst)) in enumerate(parts.items())
    }
    for load in loads.values():
        load.start()

    def gather_copy(step):
        return pltpu.make_async_remote_copy(
            src_ref=cv,
            dst_ref=cg.at[me_f],
            send_sem=g_send.at[step - 1],
            recv_sem=g_recv.at[step - 1],
            device_id=dev((me_f + step) % nf, me_r),
            device_id_type=MESH,
        )

    loads["coarse"].wait()
    pl.semaphore_wait(barrier, expected)
    for step in range(1, nf):
        gather_copy(step).start()
    cg[me_f] = cv[...]

    loads["fine"].wait()
    block = math.gcd(chans, 64)
    size = block * rows
    i = lax.broadcasted_iota(jnp.int32, (size, size), 0)
    k = lax.broadcasted_iota(jnp.int32, (size, size), 1)
    sort_rows = jnp.where((k % rows == i // block) & (k // rows == i % block), 1.0, 0.0).astype(BF)
    for b in range(chans // block):
        mixed_rows = jnp.concatenate([ff[t, b * size : (b + 1) * size, :] for t in range(f_dev)], axis=1)
        sorted_rows = dot(sort_rows, mixed_rows).astype(BF)
        for t in range(f_dev):
            for r in range(rows):
                fb[1 + t, 1 + r, b * block : (b + 1) * block, :] = sorted_rows[
                    r * block : (r + 1) * block, t * width : (t + 1) * width
                ]

    def remote(n, src, dst, f, r):
        return pltpu.make_async_remote_copy(
            src_ref=src,
            dst_ref=dst,
            send_sem=halo_send.at[n],
            recv_sem=halo_recv.at[n],
            device_id=dev(f, r),
            device_id_type=MESH,
        )

    own_f = pl.ds(1, f_dev)
    row_order = [0, rows - 1, *range(1, rows - 1)] if rows > 1 else [0]
    row_halo, corner_halo = [], []
    frame_halo = [[] for _ in row_order]
    at_frame = ((0, me_f > 0), (frames_ext - 1, me_f < nf - 1))
    n_sem = 0
    for d in (-1, 1):
        there = (me_r + d >= 0) & (me_r + d < nr)
        source = (me_r - d >= 0) & (me_r - d < nr)
        src_r, dst_r = (rows, 0) if d > 0 else (1, rows_ext - 1)
        row_halo.append(
            (remote(n_sem, fb.at[own_f, src_r], fb.at[own_f, dst_r], me_f, me_r + d), there, source)
        )
        n_sem += 1
        for at, exists in at_frame:
            corner_halo.append(
                (remote(n_sem, fb.at[at, src_r], fb.at[at, dst_r], me_f, me_r + d), there & exists, source & exists)
            )
            n_sem += 1
    for d in (-1, 1):
        there = (me_f + d >= 0) & (me_f + d < nf)
        source = (me_f - d >= 0) & (me_f - d < nf)
        src_f, dst_f = (f_dev, 0) if d > 0 else (1, frames_ext - 1)
        for place, r in enumerate(row_order):
            copy = remote(n_sem, fb.at[src_f, 1 + r], fb.at[dst_f, 1 + r], me_f + d, me_r)
            frame_halo[place].append((copy, there, source))
            n_sem += 1

    def start_all(copies):
        for copy, there, _ in copies:

            @pl.when(there)
            def _(copy=copy):
                copy.start()

    def arrive_all(copies):
        for copy, _, source in copies:

            @pl.when(source)
            def _(copy=copy):
                copy.wait_recv()

    def sent_all(copies):
        for copy, there, _ in copies:

            @pl.when(there)
            def _(copy=copy):
                copy.wait_send()

    start_all(row_halo)
    start_all(frame_halo[0])
    if rows > 1:
        start_all(frame_halo[1])

    for edge, at in ((me_r == 0, 0), (me_r == nr - 1, rows_ext - 1)):

        @pl.when(edge)
        def _(at=at):
            fb[:, at] = jnp.zeros((frames_ext, chans, width), BF)

    for edge, at in ((me_f == 0, 0), (me_f == nf - 1, frames_ext - 1)):

        @pl.when(edge)
        def _(at=at):
            fb[at] = jnp.zeros((rows_ext, chans, width), BF)

    for edge, region in ((first & (my_group == 0), 1), (last & (my_group == n_groups - 1), 2)):

        @pl.when(edge)
        def _(region=region):
            ub[:, region] = jnp.zeros((3, span, chans), BF)

    for edge, slot in ((me_f == 0, 1), (me_f == nf - 1, 2)):

        @pl.when(edge)
        def _(slot=slot):
            ub[slot] = jnp.zeros((3, span, chans), BF)

    loads["gain_one"].wait()
    loads["gain_two"].wait()
    half_one[...] = jnp.broadcast_to(0.5 * g1[...][None, :], (width, chans)).T
    half_two[...] = jnp.broadcast_to(0.5 * g2[...][None, :], (width, chans)).T

    def turn(dy):
        loads[f"space{dy}"].wait()
        cst[dy] = cs[dy].T

    loads["qkv"].wait()
    turn(0)
    for step in range(1, nf):
        gather_copy(step).wait()
    cells_all = jnp.concatenate([cg[j].astype(F32) for j in range(nf)], axis=1).astype(BF)
    qkv = []
    for i in range(3):
        product = lax.dot_general(
            cells_all, wq[i], (((1,), (1,)), ((), ())), preferred_element_type=F32
        )
        qkv.append(product.astype(BF))
    query, keys, values = qkv

    head_of_lane = lax.broadcasted_iota(jnp.int32, (cells, c_dev), 1) // HD
    spread = jnp.concatenate(
        [jnp.where(head_of_lane == h, query.astype(F32), 0.0) for h in range(heads)], axis=0
    ).astype(BF)
    scores = lax.dot_general(
        spread, keys, (((1,), (1,)), ((), ())), preferred_element_type=F32
    ) / math.sqrt(HD)
    cell_q = lax.broadcasted_iota(jnp.int32, scores.shape, 0) % p_dev
    cell_k = lax.broadcasted_iota(jnp.int32, scores.shape, 1) % p_dev
    same = cell_q == cell_k
    scores = jnp.where(same, scores, -1e30)
    top = jnp.max(scores, axis=1, keepdims=True)
    weight = jnp.where(same, jnp.exp(scores - top), 0.0)
    probs = (weight / jnp.sum(weight, axis=1, keepdims=True)).astype(BF)
    mixed = dot(probs, values)
    attn = None
    for h in range(heads):
        part = jnp.where(head_of_lane == h, mixed[h * cells : (h + 1) * cells], 0.0)
        attn = part if attn is None else attn + part
    attn = attn.astype(BF)

    loads["out"].wait()
    partial_out = dot(attn, wo[...])
    for j in range(nf):
        rs_send[j] = partial_out[:, j * c_dev : (j + 1) * c_dev].astype(BF)

    def scatter_copy(step):
        peer = (me_f + step) % nf
        return pltpu.make_async_remote_copy(
            src_ref=rs_send.at[peer],
            dst_ref=rs_recv.at[me_f],
            send_sem=r_send.at[step - 1],
            recv_sem=r_recv.at[step - 1],
            device_id=dev(peer, me_r),
            device_id_type=MESH,
        )

    for step in range(1, nf):
        scatter_copy(step).start()
    if rows > 2:
        start_all(frame_halo[2])
    rs_recv[me_f] = rs_send[me_f]
    turn(1)
    loads["up"].wait()
    for step in range(1, nf):
        scatter_copy(step).wait()
    share = cv[...].astype(F32)
    for j in range(nf):
        share = share + rs_recv[j].astype(F32)
    up_partial = dot(share.astype(BF), wu[...])
    for j in range(cf_count):
        up_send[j] = up_partial[j * p_dev : (j + 1) * p_dev].astype(BF)

    def coarse_frame(f):
        return (f * f_dev * cf_count) // total_frames

    def sum_copy(step_f, step_k):
        peer = (me_f + step_f) % nf
        return pltpu.make_async_remote_copy(
            src_ref=up_send.at[coarse_frame(peer)],
            dst_ref=up_recv.at[k_me, me_f],
            send_sem=u_send.at[step_f, step_k],
            recv_sem=u_recv.at[step_f, step_k],
            device_id=dev(peer, base + (k_me + step_k) % group),
            device_id_type=MESH,
        )

    sums = [(a, b) for a in range(nf) for b in range(group) if a or b]
    for a, b in sums[::-1]:
        sum_copy(a, b).start()
    up_recv[k_me, me_f] = up_send[coarse_frame(me_f)]
    for place in range(3, rows):
        start_all(frame_halo[place])
    arrive_all(frame_halo[0])
    if rows > 1:
        arrive_all(frame_halo[1])
    start_all(corner_halo)
    turn(2)
    loads["time"].wait()
    ctt[...] = ct[...].T
    rho = lax.broadcasted_iota(jnp.int32, (span, width), 0)
    lane = lax.broadcasted_iota(jnp.int32, (span, width), 1)
    pick = jnp.where(lane // UPSAMPLE == rho, 1.0, 0.0).astype(BF)
    for a, b in sums:
        sum_copy(a, b).wait()
    halves = []
    for c in range(group):
        up = up_recv[c, 0].astype(F32)
        for j in range(1, nf):
            up = up + up_recv[c, j].astype(F32)
        halves.append(up)
    ub[0, 0] = (jnp.concatenate(halves, axis=0) if group > 1 else halves[0]).astype(BF)

    def block_copy(n, src, slot, region, f, r):
        return pltpu.make_async_remote_copy(
            src_ref=ub.at[0, src],
            dst_ref=ub.at[slot, region],
            send_sem=b_send.at[n],
            recv_sem=b_recv.at[slot, region],
            device_id=dev(f, r),
            device_id_type=MESH,
        )

    edges = [
        (block_copy(0, 0, 0, 1, me_f, me_r + 1), has_below, has_above),
        (block_copy(1, 0, 0, 2, me_f, me_r - 1), has_above, has_below),
    ]
    beside = []
    n_block = 2
    for slot, d in ((1, 1), (2, -1)):
        there = (me_f + d >= 0) & (me_f + d < nf)
        source = (me_f - d >= 0) & (me_f - d < nf)
        for region, have in ((0, None), (1, has_above), (2, has_below)):
            copy = block_copy(n_block, region, slot, region, me_f + d, me_r)
            n_block += 1
            beside.append((copy, there, source) if have is None else (copy, there & have, source & have))
    start_all(edges)
    start_all(beside[::3])

    lane_bf = lax.broadcasted_iota(jnp.int32, (chans, width), 1)
    keep_left = jnp.where(lane_bf == 0, 0.0, 1.0).astype(BF)
    keep_right = jnp.where(lane_bf == width - 1, 0.0, 1.0).astype(BF)

    def activate(t, r, widened):
        v = fb[t, r].astype(F32) + widened
        if 0 < t < frames_ext - 1 and 0 < r < rows_ext - 1:
            mg[t - 1, r - 1] = v.astype(BF)
        act = norm_silu(v, half_one[...]).astype(BF)
        here = slice(r * width, (r + 1) * width)
        x3[t, chans : 2 * chans, here] = act
        x3[t, 0:chans, here] = pltpu.roll(act, 1, 1) * keep_left
        x3[t, 2 * chans : 3 * chans, here] = pltpu.roll(act, width - 1, 1) * keep_right

    def convolve(t):
        spatial = None
        for dy in range(3):
            term = dot(cst[dy], x3[t, :, dy * width : (dy + rows) * width])
            spatial = term if spatial is None else spatial + term
        for r in range(rows):
            here = slice(r * width, (r + 1) * width)
            n2[t * chans : (t + 1) * chans, here] = norm_silu(spatial[:, here], half_two[...]).astype(BF)

    own = dot_t(ub[0, 0], pick)
    for t in range(1, frames_ext - 1):
        for r in range(1, rows_ext - 1):
            activate(t, r, own)
    arrive_all(edges)
    start_all(beside[1::3])
    start_all(beside[2::3])
    arrive_all(row_halo)
    above = dot_t(ub[0, jnp.where(first, 1, 0)], pick)
    below = dot_t(ub[0, jnp.where(last, 2, 0)], pick)
    for t in range(1, frames_ext - 1):
        activate(t, 0, above)
        activate(t, rows_ext - 1, below)
    for t in range(1, frames_ext - 1):
        convolve(t)
    for place in range(2, rows):
        arrive_all(frame_halo[place])
    arrive_all(beside)
    arrive_all(corner_halo)
    for t, slot in ((0, 1), (frames_ext - 1, 2)):
        own = dot_t(ub[slot, 0], pick)
        above = dot_t(ub[slot, jnp.where(first, 1, 0)], pick)
        below = dot_t(ub[slot, jnp.where(last, 2, 0)], pick)
        for r in range(rows_ext):
            activate(t, r, above if r == 0 else below if r == rows_ext - 1 else own)
        convolve(t)
    outs = []
    for t in range(f_dev):
        temporal = dot(ctt[...], n2[t * chans : (t + 3) * chans, :])
        for r in range(rows):
            here = slice(r * width, (r + 1) * width)
            o32[t, pl.ds(r, chans, rows), :] = mg[t, r].astype(F32) + temporal[:, here]
        ov[t] = o32[t].astype(BF)
        outs.append(pltpu.make_async_copy(ov.at[t], out_ref.at[t], out_sem.at[t]))
        outs[t].start()

    for copies in (row_halo, *frame_halo, corner_halo, edges, beside):
        sent_all(copies)
    for copy in outs:
        copy.wait()


def local(fine, coarse, w_qkv, w_out, w_up, gain_one, conv_space, gain_two, conv_time):
    nf = lax.axis_size("frame")
    nr = lax.axis_size("row")
    f_dev, chans, rows, width = fine.shape
    cf_count, p_dev, c_dev = coarse.shape
    cells = cf_count * p_dev
    cc = nf * c_dev
    group = (width // UPSAMPLE) // p_dev
    span = group * p_dev
    any_spec = pl.BlockSpec(memory_space=pl.ANY)
    dma = pltpu.SemaphoreType.DMA
    n_halo = 2 * (1 + 2) + 2 * rows
    out = pl.pallas_call(
        functools.partial(kernel, nf, nr, cf_count, p_dev, rows),
        out_shape=jax.ShapeDtypeStruct((f_dev, chans * rows, width), BF),
        in_specs=[any_spec] * 9,
        out_specs=any_spec,
        scratch_shapes=[
            pltpu.VMEM((cells, c_dev), BF),
            pltpu.VMEM((chans,), F32),
            pltpu.VMEM((chans,), F32),
            pltpu.VMEM((f_dev, chans * rows, width), BF),
            pltpu.VMEM((3, c_dev, cc), BF),
            pltpu.VMEM((c_dev, cc), BF),
            pltpu.VMEM((c_dev, chans), BF),
            pltpu.VMEM((3, 3 * chans, chans), BF),
            pltpu.VMEM((3 * chans, chans), BF),
            pltpu.VMEM((3, chans, 3 * chans), BF),
            pltpu.VMEM((chans, 3 * chans), BF),
            pltpu.VMEM((f_dev + 2, rows + 2, chans, width), BF),
            pltpu.VMEM((f_dev, rows, chans, width), BF),
            pltpu.VMEM((nf, cells, c_dev), BF),
            pltpu.VMEM((nf, cells, c_dev), BF),
            pltpu.VMEM((nf, cells, c_dev), BF),
            pltpu.VMEM((cf_count, p_dev, chans), BF),
            pltpu.VMEM((group, nf, p_dev, chans), BF),
            pltpu.VMEM((3, 3, span, chans), BF),
            pltpu.VMEM((f_dev + 2, 3 * chans, (rows + 2) * width), BF),
            pltpu.VMEM(((f_dev + 2) * chans, rows * width), BF),
            pltpu.VMEM((chans, width), F32),
            pltpu.VMEM((chans, width), F32),
            pltpu.VMEM((f_dev, chans * rows, width), F32),
            pltpu.VMEM((f_dev, chans * rows, width), BF),
            dma((11,)),
            dma((n_halo,)),
            dma((n_halo,)),
            dma((nf,)),
            dma((nf,)),
            dma((nf,)),
            dma((nf,)),
            dma((nf, group)),
            dma((nf, group)),
            dma((8,)),
            dma((3, 3)),
            dma((f_dev,)),
        ],
        compiler_params=pltpu.CompilerParams(
            collective_id=0, has_side_effects=True, vmem_limit_bytes=56 * 1024 * 1024
        ),
        name="decoder_window",
    )(
        fine.reshape(f_dev, chans * rows, width),
        coarse.reshape(cells, c_dev),
        jnp.swapaxes(w_qkv, 1, 2),
        w_out,
        w_up,
        gain_one,
        conv_space.reshape(3, 3 * chans, chans),
        gain_two,
        conv_time.reshape(3 * chans, chans),
    )
    return out.reshape(f_dev, chans, rows, width)


def solution(mesh):
    return jax.shard_map(
        local,
        mesh=mesh,
        in_specs=(
            P("frame", None, "row", None),
            P(None, "row", "frame"),
            P(None, None, "frame"),
            P("frame", None),
            P("frame", None),
            P(),
            P(),
            P(),
            P(),
        ),
        out_specs=P("frame", None, "row", None),
        check_vma=False,
    )
```

```python
import functools
import math

import jax
import jax.numpy as jnp
from jax import lax
from jax.experimental import pallas as pl
from jax.experimental.pallas import tpu as pltpu
from jax.sharding import PartitionSpec as P

HD = 80
UPSAMPLE = 8
MESH = pl.DeviceIdType.MESH
BF = jnp.bfloat16
F32 = jnp.float32


def dot(a, b):
    return jnp.dot(a, b, preferred_element_type=F32)


def dot_t(a, b):
    return lax.dot_general(a, b, (((0,), (0,)), ((), ())), preferred_element_type=F32)


def norm_silu(v, half_gain):
    scale = lax.rsqrt(jnp.mean(v * v, axis=0, keepdims=True) + 1e-06)
    half = v * scale * half_gain
    return half + half * jnp.tanh(half)


def kernel(
    nf, nr, cf_count, p_dev, rows,
    fine_ref, coarse_ref, w_qkv_ref, w_out_ref, w_up_ref, gain_one_ref, conv_s_ref, gain_two_ref, conv_t_ref,
    out_ref,
    cv, g1, g2, ff, wq, wo, wu, cs, ct, cst, ctt, fb, mg, cg, rs_send, rs_recv, up_send, up_recv, ub, x3, n2,
    half_one, half_two, o32,
    load_sem, halo_send, halo_recv, g_send, g_recv, r_send, r_recv, u_send, u_recv, b_send, b_recv,
):
    f_dev, flat, width = fine_ref.shape
    chans = flat // rows
    cells, c_dev = coarse_ref.shape
    frames_ext = f_dev + 2
    rows_ext = rows + 2
    group = (width // UPSAMPLE) // p_dev
    n_groups = nr // group
    heads = c_dev // HD
    span = group * p_dev
    total_frames = nf * f_dev
    me_f = lax.axis_index("frame")
    me_r = lax.axis_index("row")
    my_group = me_r // group
    k_me = me_r % group
    base = my_group * group
    first = k_me == 0
    last = k_me == group - 1
    has_above = first & (my_group > 0)
    has_below = last & (my_group < n_groups - 1)

    def dev(f, r):
        return {"frame": f, "row": r}

    barrier = pltpu.get_barrier_semaphore()
    for step_f in range(nf):
        for step_k in range(group):
            if step_f or step_k:
                peer = dev((me_f + step_f) % nf, base + (k_me + step_k) % group)
                pl.semaphore_signal(barrier, inc=1, device_id=peer, device_id_type=MESH)
    expected = jnp.int32(nf * group - 1)
    for ok, peer in ((has_above, me_r - 1), (has_below, me_r + 1)):
        expected = expected + ok.astype(jnp.int32)

        @pl.when(ok)
        def _(peer=peer):
            pl.semaphore_signal(barrier, inc=1, device_id=dev(me_f, peer), device_id_type=MESH)

    parts = {
        "coarse": (coarse_ref, cv),
        "fine": (fine_ref, ff),
        "gain_one": (gain_one_ref, g1),
        "gain_two": (gain_two_ref, g2),
        "qkv": (w_qkv_ref, wq),
        "out": (w_out_ref, wo),
        "space0": (conv_s_ref.at[0], cs.at[0]),
        "up": (w_up_ref, wu),
        "space1": (conv_s_ref.at[1], cs.at[1]),
        "space2": (conv_s_ref.at[2], cs.at[2]),
        "time": (conv_t_ref, ct),
    }
    loads = {
        name: pltpu.make_async_copy(src, dst, load_sem.at[n])
        for n, (name, (src, dst)) in enumerate(parts.items())
    }
    for load in loads.values():
        load.start()

    def gather_copy(step):
        return pltpu.make_async_remote_copy(
            src_ref=cv,
            dst_ref=cg.at[me_f],
            send_sem=g_send.at[step - 1],
            recv_sem=g_recv.at[step - 1],
            device_id=dev((me_f + step) % nf, me_r),
            device_id_type=MESH,
        )

    loads["coarse"].wait()
    pl.semaphore_wait(barrier, expected)
    for step in range(1, nf):
        gather_copy(step).start()
    cg[me_f] = cv[...]

    loads["fine"].wait()
    block = math.gcd(chans, 64)
    size = block * rows
    i = lax.broadcasted_iota(jnp.int32, (size, size), 0)
    k = lax.broadcasted_iota(jnp.int32, (size, size), 1)
    sort_rows = jnp.where((k % rows == i // block) & (k // rows == i % block), 1.0, 0.0).astype(BF)
    for b in range(chans // block):
        mixed_rows = jnp.concatenate([ff[t, b * size : (b + 1) * size, :] for t in range(f_dev)], axis=1)
        sorted_rows = dot(sort_rows, mixed_rows).astype(BF)
        for t in range(f_dev):
            for r in range(rows):
                fb[1 + t, 1 + r, b * block : (b + 1) * block, :] = sorted_rows[
                    r * block : (r + 1) * block, t * width : (t + 1) * width
                ]

    def remote(n, src, dst, f, r):
        return pltpu.make_async_remote_copy(
            src_ref=src,
            dst_ref=dst,
            send_sem=halo_send.at[n],
            recv_sem=halo_recv.at[n],
            device_id=dev(f, r),
            device_id_type=MESH,
        )

    own_f = pl.ds(1, f_dev)
    row_order = [0, rows - 1, *range(1, rows - 1)] if rows > 1 else [0]
    row_halo, corner_halo = [], []
    frame_halo = [[] for _ in row_order]
    at_frame = ((0, me_f > 0), (frames_ext - 1, me_f < nf - 1))
    n_sem = 0
    for d in (-1, 1):
        there = (me_r + d >= 0) & (me_r + d < nr)
        source = (me_r - d >= 0) & (me_r - d < nr)
        src_r, dst_r = (rows, 0) if d > 0 else (1, rows_ext - 1)
        row_halo.append(
            (remote(n_sem, fb.at[own_f, src_r], fb.at[own_f, dst_r], me_f, me_r + d), there, source)
        )
        n_sem += 1
        for at, exists in at_frame:
            corner_halo.append(
                (remote(n_sem, fb.at[at, src_r], fb.at[at, dst_r], me_f, me_r + d), there & exists, source & exists)
            )
            n_sem += 1
    for d in (-1, 1):
        there = (me_f + d >= 0) & (me_f + d < nf)
        source = (me_f - d >= 0) & (me_f - d < nf)
        src_f, dst_f = (f_dev, 0) if d > 0 else (1, frames_ext - 1)
        for place, r in enumerate(row_order):
            copy = remote(n_sem, fb.at[src_f, 1 + r], fb.at[dst_f, 1 + r], me_f + d, me_r)
            frame_halo[place].append((copy, there, source))
            n_sem += 1

    def start_all(copies):
        for copy, there, _ in copies:

            @pl.when(there)
            def _(copy=copy):
                copy.start()

    def arrive_all(copies):
        for copy, _, source in copies:

            @pl.when(source)
            def _(copy=copy):
                copy.wait_recv()

    def sent_all(copies):
        for copy, there, _ in copies:

            @pl.when(there)
            def _(copy=copy):
                copy.wait_send()

    start_all(row_halo)
    start_all(frame_halo[0])
    if rows > 1:
        start_all(frame_halo[1])

    for edge, at in ((me_r == 0, 0), (me_r == nr - 1, rows_ext - 1)):

        @pl.when(edge)
        def _(at=at):
            fb[:, at] = jnp.zeros((frames_ext, chans, width), BF)

    for edge, at in ((me_f == 0, 0), (me_f == nf - 1, frames_ext - 1)):

        @pl.when(edge)
        def _(at=at):
            fb[at] = jnp.zeros((rows_ext, chans, width), BF)

    for edge, region in ((first & (my_group == 0), 1), (last & (my_group == n_groups - 1), 2)):

        @pl.when(edge)
        def _(region=region):
            ub[:, region] = jnp.zeros((3, span, chans), BF)

    for edge, slot in ((me_f == 0, 1), (me_f == nf - 1, 2)):

        @pl.when(edge)
        def _(slot=slot):
            ub[slot] = jnp.zeros((3, span, chans), BF)

    loads["gain_one"].wait()
    loads["gain_two"].wait()
    half_one[...] = jnp.broadcast_to(0.5 * g1[...][None, :], (width, chans)).T
    half_two[...] = jnp.broadcast_to(0.5 * g2[...][None, :], (width, chans)).T

    def turn(dy):
        loads[f"space{dy}"].wait()
        cst[dy] = cs[dy].T

    loads["qkv"].wait()
    turn(0)
    for step in range(1, nf):
        gather_copy(step).wait()
    cells_all = jnp.concatenate([cg[j].astype(F32) for j in range(nf)], axis=1).astype(BF)
    qkv = []
    for i in range(3):
        product = lax.dot_general(
            cells_all, wq[i], (((1,), (1,)), ((), ())), preferred_element_type=F32
        )
        qkv.append(product.astype(BF))
    query, keys, values = qkv

    head_of_lane = lax.broadcasted_iota(jnp.int32, (cells, c_dev), 1) // HD
    spread = jnp.concatenate(
        [jnp.where(head_of_lane == h, query.astype(F32), 0.0) for h in range(heads)], axis=0
    ).astype(BF)
    scores = lax.dot_general(
        spread, keys, (((1,), (1,)), ((), ())), preferred_element_type=F32
    ) / math.sqrt(HD)
    cell_q = lax.broadcasted_iota(jnp.int32, scores.shape, 0) % p_dev
    cell_k = lax.broadcasted_iota(jnp.int32, scores.shape, 1) % p_dev
    same = cell_q == cell_k
    scores = jnp.where(same, scores, -1e30)
    top = jnp.max(scores, axis=1, keepdims=True)
    weight = jnp.where(same, jnp.exp(scores - top), 0.0)
    probs = (weight / jnp.sum(weight, axis=1, keepdims=True)).astype(BF)
    mixed = dot(probs, values)
    attn = None
    for h in range(heads):
        part = jnp.where(head_of_lane == h, mixed[h * cells : (h + 1) * cells], 0.0)
        attn = part if attn is None else attn + part
    attn = attn.astype(BF)

    loads["out"].wait()
    partial_out = dot(attn, wo[...])
    for j in range(nf):
        rs_send[j] = partial_out[:, j * c_dev : (j + 1) * c_dev].astype(BF)

    def scatter_copy(step):
        peer = (me_f + step) % nf
        return pltpu.make_async_remote_copy(
            src_ref=rs_send.at[peer],
            dst_ref=rs_recv.at[me_f],
            send_sem=r_send.at[step - 1],
            recv_sem=r_recv.at[step - 1],
            device_id=dev(peer, me_r),
            device_id_type=MESH,
        )

    for step in range(1, nf):
        scatter_copy(step).start()
    if rows > 2:
        start_all(frame_halo[2])
    rs_recv[me_f] = rs_send[me_f]
    turn(1)
    loads["up"].wait()
    for step in range(1, nf):
        scatter_copy(step).wait()
    share = cv[...].astype(F32)
    for j in range(nf):
        share = share + rs_recv[j].astype(F32)
    up_partial = dot(share.astype(BF), wu[...])
    for j in range(cf_count):
        up_send[j] = up_partial[j * p_dev : (j + 1) * p_dev].astype(BF)

    def coarse_frame(f):
        return (f * f_dev * cf_count) // total_frames

    def sum_copy(step_f, step_k):
        peer = (me_f + step_f) % nf
        return pltpu.make_async_remote_copy(
            src_ref=up_send.at[coarse_frame(peer)],
            dst_ref=up_recv.at[k_me, me_f],
            send_sem=u_send.at[step_f, step_k],
            recv_sem=u_recv.at[step_f, step_k],
            device_id=dev(peer, base + (k_me + step_k) % group),
            device_id_type=MESH,
        )

    sums = [(a, b) for a in range(nf) for b in range(group) if a or b]
    for a, b in sums[::-1]:
        sum_copy(a, b).start()
    up_recv[k_me, me_f] = up_send[coarse_frame(me_f)]
    for place in range(3, rows):
        start_all(frame_halo[place])
    arrive_all(frame_halo[0])
    if rows > 1:
        arrive_all(frame_halo[1])
    start_all(corner_halo)
    turn(2)
    loads["time"].wait()
    ctt[...] = ct[...].T
    rho = lax.broadcasted_iota(jnp.int32, (span, width), 0)
    lane = lax.broadcasted_iota(jnp.int32, (span, width), 1)
    pick = jnp.where(lane // UPSAMPLE == rho, 1.0, 0.0).astype(BF)
    for a, b in sums:
        sum_copy(a, b).wait()
    halves = []
    for c in range(group):
        up = up_recv[c, 0].astype(F32)
        for j in range(1, nf):
            up = up + up_recv[c, j].astype(F32)
        halves.append(up)
    ub[0, 0] = (jnp.concatenate(halves, axis=0) if group > 1 else halves[0]).astype(BF)

    def block_copy(n, src, slot, region, f, r):
        return pltpu.make_async_remote_copy(
            src_ref=ub.at[0, src],
            dst_ref=ub.at[slot, region],
            send_sem=b_send.at[n],
            recv_sem=b_recv.at[slot, region],
            device_id=dev(f, r),
            device_id_type=MESH,
        )

    edges = [
        (block_copy(0, 0, 0, 1, me_f, me_r + 1), has_below, has_above),
        (block_copy(1, 0, 0, 2, me_f, me_r - 1), has_above, has_below),
    ]
    beside = []
    n_block = 2
    for slot, d in ((1, 1), (2, -1)):
        there = (me_f + d >= 0) & (me_f + d < nf)
        source = (me_f - d >= 0) & (me_f - d < nf)
        for region, have in ((0, None), (1, has_above), (2, has_below)):
            copy = block_copy(n_block, region, slot, region, me_f + d, me_r)
            n_block += 1
            beside.append((copy, there, source) if have is None else (copy, there & have, source & have))
    start_all(edges)
    start_all(beside[::3])

    lane_bf = lax.broadcasted_iota(jnp.int32, (chans, width), 1)
    keep_left = jnp.where(lane_bf == 0, 0.0, 1.0).astype(BF)
    keep_right = jnp.where(lane_bf == width - 1, 0.0, 1.0).astype(BF)

    def activate(t, r, widened):
        v = fb[t, r].astype(F32) + widened
        if 0 < t < frames_ext - 1 and 0 < r < rows_ext - 1:
            mg[t - 1, r - 1] = v.astype(BF)
        act = norm_silu(v, half_one[...]).astype(BF)
        here = slice(r * width, (r + 1) * width)
        x3[t, chans : 2 * chans, here] = act
        x3[t, 0:chans, here] = pltpu.roll(act, 1, 1) * keep_left
        x3[t, 2 * chans : 3 * chans, here] = pltpu.roll(act, width - 1, 1) * keep_right

    def convolve(t):
        spatial = None
        for dy in range(3):
            term = dot(cst[dy], x3[t, :, dy * width : (dy + rows) * width])
            spatial = term if spatial is None else spatial + term
        for r in range(rows):
            here = slice(r * width, (r + 1) * width)
            n2[t * chans : (t + 1) * chans, here] = norm_silu(spatial[:, here], half_two[...]).astype(BF)

    own = dot_t(ub[0, 0], pick)
    for t in range(1, frames_ext - 1):
        for r in range(1, rows_ext - 1):
            activate(t, r, own)
    arrive_all(edges)
    start_all(beside[1::3])
    start_all(beside[2::3])
    arrive_all(row_halo)
    above = dot_t(ub[0, jnp.where(first, 1, 0)], pick)
    below = dot_t(ub[0, jnp.where(last, 2, 0)], pick)
    for t in range(1, frames_ext - 1):
        activate(t, 0, above)
        activate(t, rows_ext - 1, below)
    for t in range(1, frames_ext - 1):
        convolve(t)
    for place in range(2, rows):
        arrive_all(frame_halo[place])
    arrive_all(beside)
    arrive_all(corner_halo)
    for t, slot in ((0, 1), (frames_ext - 1, 2)):
        own = dot_t(ub[slot, 0], pick)
        above = dot_t(ub[slot, jnp.where(first, 1, 0)], pick)
        below = dot_t(ub[slot, jnp.where(last, 2, 0)], pick)
        for r in range(rows_ext):
            activate(t, r, above if r == 0 else below if r == rows_ext - 1 else own)
        convolve(t)
    for t in range(f_dev):
        temporal = dot(ctt[...], n2[t * chans : (t + 3) * chans, :])
        for r in range(rows):
            here = slice(r * width, (r + 1) * width)
            o32[t, pl.ds(r, chans, rows), :] = mg[t, r].astype(F32) + temporal[:, here]
        out_ref[t] = o32[t].astype(BF)

    for copies in (row_halo, *frame_halo, corner_halo, edges, beside):
        sent_all(copies)


def local(fine, coarse, w_qkv, w_out, w_up, gain_one, conv_space, gain_two, conv_time):
    nf = lax.axis_size("frame")
    nr = lax.axis_size("row")
    f_dev, chans, rows, width = fine.shape
    cf_count, p_dev, c_dev = coarse.shape
    cells = cf_count * p_dev
    cc = nf * c_dev
    group = (width // UPSAMPLE) // p_dev
    span = group * p_dev
    any_spec = pl.BlockSpec(memory_space=pl.ANY)
    dma = pltpu.SemaphoreType.DMA
    n_halo = 2 * (1 + 2) + 2 * rows
    out = pl.pallas_call(
        functools.partial(kernel, nf, nr, cf_count, p_dev, rows),
        out_shape=pltpu.VMEM((f_dev, chans * rows, width), BF),
        in_specs=[any_spec] * 9,
        out_specs=pl.BlockSpec(memory_space=pltpu.VMEM),
        scratch_shapes=[
            pltpu.VMEM((cells, c_dev), BF),
            pltpu.VMEM((chans,), F32),
            pltpu.VMEM((chans,), F32),
            pltpu.VMEM((f_dev, chans * rows, width), BF),
            pltpu.VMEM((3, c_dev, cc), BF),
            pltpu.VMEM((c_dev, cc), BF),
            pltpu.VMEM((c_dev, chans), BF),
            pltpu.VMEM((3, 3 * chans, chans), BF),
            pltpu.VMEM((3 * chans, chans), BF),
            pltpu.VMEM((3, chans, 3 * chans), BF),
            pltpu.VMEM((chans, 3 * chans), BF),
            pltpu.VMEM((f_dev + 2, rows + 2, chans, width), BF),
            pltpu.VMEM((f_dev, rows, chans, width), BF),
            pltpu.VMEM((nf, cells, c_dev), BF),
            pltpu.VMEM((nf, cells, c_dev), BF),
            pltpu.VMEM((nf, cells, c_dev), BF),
            pltpu.VMEM((cf_count, p_dev, chans), BF),
            pltpu.VMEM((group, nf, p_dev, chans), BF),
            pltpu.VMEM((3, 3, span, chans), BF),
            pltpu.VMEM((f_dev + 2, 3 * chans, (rows + 2) * width), BF),
            pltpu.VMEM(((f_dev + 2) * chans, rows * width), BF),
            pltpu.VMEM((chans, width), F32),
            pltpu.VMEM((chans, width), F32),
            pltpu.VMEM((f_dev, chans * rows, width), F32),
            dma((11,)),
            dma((n_halo,)),
            dma((n_halo,)),
            dma((nf,)),
            dma((nf,)),
            dma((nf,)),
            dma((nf,)),
            dma((nf, group)),
            dma((nf, group)),
            dma((8,)),
            dma((3, 3)),
        ],
        compiler_params=pltpu.CompilerParams(
            collective_id=0, has_side_effects=True, vmem_limit_bytes=56 * 1024 * 1024
        ),
        name="decoder_window",
    )(
        fine.reshape(f_dev, chans * rows, width),
        coarse.reshape(cells, c_dev),
        jnp.swapaxes(w_qkv, 1, 2),
        w_out,
        w_up,
        gain_one,
        conv_space.reshape(3, 3 * chans, chans),
        gain_two,
        conv_time.reshape(3 * chans, chans),
    )
    return out.reshape(f_dev, chans, rows, width)


def solution(mesh):
    return jax.shard_map(
        local,
        mesh=mesh,
        in_specs=(
            P("frame", None, "row", None),
            P(None, "row", "frame"),
            P(None, None, "frame"),
            P("frame", None),
            P("frame", None),
            P(),
            P(),
            P(),
            P(),
        ),
        out_specs=P("frame", None, "row", None),
        check_vma=False,
    )
```

```python
import functools
import math

import jax
import jax.numpy as jnp
from jax import lax
from jax.experimental import pallas as pl
from jax.experimental.pallas import tpu as pltpu
from jax.sharding import PartitionSpec as P

HD = 80
UPSAMPLE = 8
MESH = pl.DeviceIdType.MESH
BF = jnp.bfloat16
F32 = jnp.float32


def dot(a, b):
    return jnp.dot(a, b, preferred_element_type=F32)


def dot_t(a, b):
    return lax.dot_general(a, b, (((0,), (0,)), ((), ())), preferred_element_type=F32)


def norm_silu(v, half_gain):
    scale = lax.rsqrt(jnp.mean(v * v, axis=0, keepdims=True) + 1e-06)
    half = v * scale * half_gain
    return half + half * jnp.tanh(half)


def kernel(
    nf, nr, cf_count, p_dev, rows,
    fine_ref, coarse_ref, w_qkv_ref, w_out_ref, w_up_ref, gain_one_ref, conv_s_ref, gain_two_ref, conv_t_ref,
    out_ref,
    cv, g1, g2, ff, wq, wo, wu, cs, ct, wt, fb, mg, cg, rs_send, rs_recv, up_send, up_recv, ub, x3, n2, keep, acc,
    half_one, half_two, o32,
    load_sem, halo_send, halo_recv, g_send, g_recv, r_send, r_recv, u_send, u_recv, b_send, b_recv,
):
    f_dev, flat, width = fine_ref.shape
    chans = flat // rows
    cells, c_dev = coarse_ref.shape
    frames_ext = f_dev + 2
    rows_ext = rows + 2
    group = (width // UPSAMPLE) // p_dev
    n_groups = nr // group
    heads = c_dev // HD
    span = group * p_dev
    total_frames = nf * f_dev
    me_f = lax.axis_index("frame")
    me_r = lax.axis_index("row")
    my_group = me_r // group
    k_me = me_r % group
    base = my_group * group
    first = k_me == 0
    last = k_me == group - 1
    has_above = first & (my_group > 0)
    has_below = last & (my_group < n_groups - 1)

    def dev(f, r):
        return {"frame": f, "row": r}

    barrier = pltpu.get_barrier_semaphore()
    for step_f in range(nf):
        for step_k in range(group):
            if step_f or step_k:
                peer = dev((me_f + step_f) % nf, base + (k_me + step_k) % group)
                pl.semaphore_signal(barrier, inc=1, device_id=peer, device_id_type=MESH)
    expected = jnp.int32(nf * group - 1)
    for ok, peer in ((has_above, me_r - 1), (has_below, me_r + 1)):
        expected = expected + ok.astype(jnp.int32)

        @pl.when(ok)
        def _(peer=peer):
            pl.semaphore_signal(barrier, inc=1, device_id=dev(me_f, peer), device_id_type=MESH)

    parts = {
        "coarse": (coarse_ref, cv),
        "fine": (fine_ref, ff),
        "gain_one": (gain_one_ref, g1),
        "gain_two": (gain_two_ref, g2),
        "qkv": (w_qkv_ref, wq),
        "out": (w_out_ref, wo),
        "space0": (conv_s_ref.at[0], cs.at[0]),
        "up": (w_up_ref, wu),
        "space1": (conv_s_ref.at[1], cs.at[1]),
        "space2": (conv_s_ref.at[2], cs.at[2]),
        "time": (conv_t_ref, ct),
    }
    loads = {
        name: pltpu.make_async_copy(src, dst, load_sem.at[n])
        for n, (name, (src, dst)) in enumerate(parts.items())
    }
    for load in loads.values():
        load.start()

    def start_all(copies):
        for copy, there, _ in copies:

            @pl.when(there)
            def _(copy=copy):
                copy.start()

    def arrive_all(copies):
        for copy, _, source in copies:

            @pl.when(source)
            def _(copy=copy):
                copy.wait_recv()

    def sent_all(copies):
        for copy, there, _ in copies:

            @pl.when(there)
            def _(copy=copy):
                copy.wait_send()

    def over_frames(make):
        copies = []
        for n, (far, d) in enumerate((far, d) for far in range(nf - 1, 0, -1) for d in (-1, 1)):
            there = (me_f + d * far >= 0) & (me_f + d * far < nf)
            source = (me_f - d * far >= 0) & (me_f - d * far < nf)
            copies.append((make(n, (me_f + d * far + nf) % nf), there, source))
        return copies

    gather = over_frames(
        lambda n, peer: pltpu.make_async_remote_copy(
            src_ref=cv,
            dst_ref=cg.at[me_f],
            send_sem=g_send.at[n],
            recv_sem=g_recv.at[n],
            device_id=dev(peer, me_r),
            device_id_type=MESH,
        )
    )
    loads["coarse"].wait()
    pl.semaphore_wait(barrier, expected)
    start_all(gather)
    cg[me_f] = cv[...]

    loads["fine"].wait()
    block = math.gcd(chans, 64)
    size = block * rows
    i = lax.broadcasted_iota(jnp.int32, (size, size), 0)
    k = lax.broadcasted_iota(jnp.int32, (size, size), 1)
    sort_rows = jnp.where((k % rows == i // block) & (k // rows == i % block), 1.0, 0.0).astype(BF)
    for b in range(chans // block):
        mixed_rows = jnp.concatenate([ff[t, b * size : (b + 1) * size, :] for t in range(f_dev)], axis=1)
        sorted_rows = dot(sort_rows, mixed_rows).astype(BF)
        for t in range(f_dev):
            for r in range(rows):
                fb[1 + t, 1 + r, b * block : (b + 1) * block, :] = sorted_rows[
                    r * block : (r + 1) * block, t * width : (t + 1) * width
                ]

    def remote(n, src, dst, f, r):
        return pltpu.make_async_remote_copy(
            src_ref=src,
            dst_ref=dst,
            send_sem=halo_send.at[n],
            recv_sem=halo_recv.at[n],
            device_id=dev(f, r),
            device_id_type=MESH,
        )

    own_f = pl.ds(1, f_dev)
    row_order = [0, rows - 1, *range(1, rows - 1)] if rows > 1 else [0]
    row_halo, corner_halo = [], []
    frame_halo = [[] for _ in row_order]
    at_frame = ((0, me_f > 0), (frames_ext - 1, me_f < nf - 1))
    n_sem = 0
    for d in (-1, 1):
        there = (me_r + d >= 0) & (me_r + d < nr)
        source = (me_r - d >= 0) & (me_r - d < nr)
        src_r, dst_r = (rows, 0) if d > 0 else (1, rows_ext - 1)
        row_halo.append(
            (remote(n_sem, fb.at[own_f, src_r], fb.at[own_f, dst_r], me_f, me_r + d), there, source)
        )
        n_sem += 1
        for at, exists in at_frame:
            corner_halo.append(
                (remote(n_sem, fb.at[at, src_r], fb.at[at, dst_r], me_f, me_r + d), there & exists, source & exists)
            )
            n_sem += 1
    for d in (-1, 1):
        there = (me_f + d >= 0) & (me_f + d < nf)
        source = (me_f - d >= 0) & (me_f - d < nf)
        src_f, dst_f = (f_dev, 0) if d > 0 else (1, frames_ext - 1)
        for place, r in enumerate(row_order):
            copy = remote(n_sem, fb.at[src_f, 1 + r], fb.at[dst_f, 1 + r], me_f + d, me_r)
            frame_halo[place].append((copy, there, source))
            n_sem += 1

    start_all(frame_halo[0])
    if rows > 1:
        start_all(frame_halo[1])

    for edge, at in ((me_r == 0, 0), (me_r == nr - 1, rows_ext - 1)):

        @pl.when(edge)
        def _(at=at):
            fb[:, at] = jnp.zeros((frames_ext, chans, width), BF)

    for edge, at in ((me_f == 0, 0), (me_f == nf - 1, frames_ext - 1)):

        @pl.when(edge)
        def _(at=at):
            fb[at] = jnp.zeros((rows_ext, chans, width), BF)

    for edge, region in ((first & (my_group == 0), 1), (last & (my_group == n_groups - 1), 2)):

        @pl.when(edge)
        def _(region=region):
            ub[:, region] = jnp.zeros((3, span, chans), BF)

    for edge, slot in ((me_f == 0, 1), (me_f == nf - 1, 2)):

        @pl.when(edge)
        def _(slot=slot):
            ub[slot] = jnp.zeros((3, span, chans), BF)

    loads["gain_one"].wait()
    loads["gain_two"].wait()
    half_one[...] = jnp.broadcast_to(0.5 * g1[...][None, :], (width, chans)).T
    half_two[...] = jnp.broadcast_to(0.5 * g2[...][None, :], (width, chans)).T

    pieces = [(start, min(width, 3 * chans - start)) for start in range(0, 3 * chans, width)]

    def lay(n, weights):
        for piece, (start, size) in enumerate(pieces):
            wt[n, piece, :, 0:size] = weights[start : start + size].T

    def wide(ref, n):
        return jnp.concatenate([ref[n, piece, :, 0:size] for piece, (_, size) in enumerate(pieces)], axis=1)

    loads["qkv"].wait()
    loads["space0"].wait()
    lay(0, cs[0])
    arrive_all(gather)
    cells_all = jnp.concatenate([cg[j].astype(F32) for j in range(nf)], axis=1).astype(BF)
    qkv = []
    for i in range(3):
        product = lax.dot_general(
            cells_all, wq[i], (((1,), (1,)), ((), ())), preferred_element_type=F32
        )
        qkv.append(product.astype(BF))
    query, keys, values = qkv

    head_of_lane = lax.broadcasted_iota(jnp.int32, (cells, c_dev), 1) // HD
    spread = jnp.concatenate(
        [jnp.where(head_of_lane == h, query.astype(F32), 0.0) for h in range(heads)], axis=0
    ).astype(BF)
    scores = lax.dot_general(
        spread, keys, (((1,), (1,)), ((), ())), preferred_element_type=F32
    ) / math.sqrt(HD)
    cell_q = lax.broadcasted_iota(jnp.int32, scores.shape, 0) % p_dev
    cell_k = lax.broadcasted_iota(jnp.int32, scores.shape, 1) % p_dev
    same = cell_q == cell_k
    scores = jnp.where(same, scores, -1e30)
    top = jnp.max(scores, axis=1, keepdims=True)
    weight = jnp.where(same, jnp.exp(scores - top), 0.0)
    probs = (weight / jnp.sum(weight, axis=1, keepdims=True)).astype(BF)
    mixed = dot(probs, values)
    attn = None
    for h in range(heads):
        part = jnp.where(head_of_lane == h, mixed[h * cells : (h + 1) * cells], 0.0)
        attn = part if attn is None else attn + part
    attn = attn.astype(BF)

    loads["out"].wait()
    partial_out = dot(attn, wo[...])
    for j in range(nf):
        rs_send[j] = partial_out[:, j * c_dev : (j + 1) * c_dev].astype(BF)

    scatter = over_frames(
        lambda n, peer: pltpu.make_async_remote_copy(
            src_ref=rs_send.at[peer],
            dst_ref=rs_recv.at[me_f],
            send_sem=r_send.at[n],
            recv_sem=r_recv.at[n],
            device_id=dev(peer, me_r),
            device_id_type=MESH,
        )
    )
    start_all(scatter)
    start_all(row_halo)
    rs_recv[me_f] = rs_send[me_f]
    loads["space1"].wait()
    loads["space2"].wait()
    lay(1, ((cs[0].astype(F32) + cs[2].astype(F32) + cs[1].astype(F32)) * 0.5).astype(BF))
    lay(3, cs[2])
    loads["up"].wait()
    arrive_all(scatter)
    share = cv[...].astype(F32)
    for j in range(nf):
        share = share + rs_recv[j].astype(F32)
    up_partial = dot(share.astype(BF), wu[...])
    for j in range(cf_count):
        up_send[j] = up_partial[j * p_dev : (j + 1) * p_dev].astype(BF)

    def coarse_frame(f):
        return (f * f_dev * cf_count) // total_frames

    def sum_copy(n, step_k, peer):
        return pltpu.make_async_remote_copy(
            src_ref=up_send.at[coarse_frame(peer)],
            dst_ref=up_recv.at[k_me, me_f],
            send_sem=u_send.at[n, step_k],
            recv_sem=u_recv.at[n, step_k],
            device_id=dev(peer, base + (k_me + step_k) % group),
            device_id_type=MESH,
        )

    sums = [copy for step_k in range(group) for copy in over_frames(lambda n, peer: sum_copy(n, step_k, peer))]
    sums = [sums[n + step_k * len(scatter)] for n in range(len(scatter)) for step_k in range(group)]
    for copy in sums:
        start_all([copy])
    across = [sum_copy(len(scatter), step_k, me_f) for step_k in range(1, group)]
    for copy in across:
        copy.start()
    up_recv[k_me, me_f] = up_send[coarse_frame(me_f)]
    for place in range(2, rows):
        start_all(frame_halo[place])
    arrive_all(frame_halo[0])
    if rows > 1:
        arrive_all(frame_halo[1])
    start_all(corner_halo)
    lay(2, ((cs[0].astype(F32) + cs[2].astype(F32) - cs[1].astype(F32)) * 0.5).astype(BF))
    loads["time"].wait()
    lay(4, ct[...])
    rho = lax.broadcasted_iota(jnp.int32, (span, width), 0)
    lane = lax.broadcasted_iota(jnp.int32, (span, width), 1)
    pick = jnp.where(lane // UPSAMPLE == rho, 1.0, 0.0).astype(BF)
    arrive_all(sums)
    for copy in across:
        copy.wait_recv()
    halves = []
    for c in range(group):
        up = up_recv[c, 0].astype(F32)
        for j in range(1, nf):
            up = up + up_recv[c, j].astype(F32)
        halves.append(up)
    ub[0, 0] = (jnp.concatenate(halves, axis=0) if group > 1 else halves[0]).astype(BF)

    def block_copy(n, src, slot, region, f, r):
        return pltpu.make_async_remote_copy(
            src_ref=ub.at[0, src],
            dst_ref=ub.at[slot, region],
            send_sem=b_send.at[n],
            recv_sem=b_recv.at[slot, region],
            device_id=dev(f, r),
            device_id_type=MESH,
        )

    edges = [
        (block_copy(0, 0, 0, 1, me_f, me_r + 1), has_below, has_above),
        (block_copy(1, 0, 0, 2, me_f, me_r - 1), has_above, has_below),
    ]
    beside = []
    n_block = 2
    for slot, d in ((1, 1), (2, -1)):
        there = (me_f + d >= 0) & (me_f + d < nf)
        source = (me_f - d >= 0) & (me_f - d < nf)
        for region, have in ((0, None), (1, has_above), (2, has_below)):
            copy = block_copy(n_block, region, slot, region, me_f + d, me_r)
            n_block += 1
            beside.append((copy, there, source) if have is None else (copy, there & have, source & have))
    start_all(edges)
    start_all(beside[::3])

    lane_bf = lax.broadcasted_iota(jnp.int32, (chans, width), 1)
    keep_left = jnp.where(lane_bf == 0, 0.0, 1.0).astype(BF)
    keep_right = jnp.where(lane_bf == width - 1, 0.0, 1.0).astype(BF)

    tiles = rows // 2

    def activate(t, r, widened):
        v = fb[t, r].astype(F32) + widened
        if 0 < t < frames_ext - 1 and 0 < r < rows_ext - 1:
            mg[t - 1, r - 1] = v.astype(BF)
        return norm_silu(v, half_one[...])

    def put(t, n, tile, v):
        v = v.astype(BF)
        x3[t, n, tile, chans : 2 * chans] = v
        x3[t, n, tile, 0:chans] = pltpu.roll(v, 1, 1) * keep_left
        x3[t, n, tile, 2 * chans : 3 * chans] = pltpu.roll(v, width - 1, 1) * keep_right

    def product(t, n):
        return dot(wide(wt, n), jnp.concatenate([x3[t, n, tile] for tile in range(tiles)], axis=1))

    act, term = {}, {}

    def rows_in(t, widened):
        def one(tile):
            r = 2 * tile + 1
            act[t, r] = activate(t, r, widened)
            act[t, r + 1] = activate(t, r + 1, widened)
            put(t, 1, tile, act[t, r] + act[t, r + 1])
            put(t, 2, tile, act[t, r + 1] - act[t, r])
            if tile > 0:
                put(t, 0, tile, act[t, r - 1] - act[t, r + 1])
                put(t, 3, tile - 1, act[t, r - 2] - act[t, r])
            if r + 1 == 2:
                keep[t, 0] = act[t, 2]
            if tile == tiles - 1:
                keep[t, 1] = act[t, rows - 1]

        return [functools.partial(one, tile) for tile in range(tiles)]

    def multiply(t, n):
        term[t, n] = product(t, n)
        if n == 2:
            acc[t, 0] = term[t, 1] + term[t, 2]
            acc[t, 1] = term[t, 1] - term[t, 2]

    def products(t, *which):
        return [functools.partial(multiply, t, n) for n in which]

    def ends(t, above, below):
        put(t, 0, 0, activate(t, 0, above) - keep[t, 0])
        put(t, 3, tiles - 1, keep[t, 1] - activate(t, rows_ext - 1, below))

    def second_norm(t):
        pair = (acc[t, 0] + term[t, 0], acc[t, 1] - term[t, 3])
        for r in range(rows):
            from_tile = slice((r // 2) * width, (r // 2 + 1) * width)
            n2[r, t * chans : (t + 1) * chans] = norm_silu(pair[r % 2][:, from_tile], half_two[...]).astype(BF)

    def temporal(t):
        window = jnp.concatenate([n2[r, t * chans : (t + 3) * chans] for r in range(rows)], axis=1)
        term[t] = dot(wide(wt, 4), window)

    def finish(t):
        for r in range(rows):
            here = slice(r * width, (r + 1) * width)
            o32[t, pl.ds(r, chans, rows), :] = mg[t, r].astype(F32) + term[t][:, here]
        out_ref[t] = o32[t].astype(BF)

    def weave(first_list, second_list):
        for n in range(max(len(first_list), len(second_list))):
            for steps in (first_list, second_list):
                if n < len(steps):
                    steps[n]()

    def sides(slot):
        return (
            dot_t(ub[slot, jnp.where(first, 1, 0)], pick),
            dot_t(ub[slot, jnp.where(last, 2, 0)], pick),
        )

    beside_frames = ((0, 1), (frames_ext - 1, 2))
    own = dot_t(ub[0, 0], pick)
    own_frames = range(1, frames_ext - 1)
    before = []
    for t in own_frames:
        weave(before, rows_in(t, own))
        before = products(t, 1, 2)
    weave(before, [])
    arrive_all(edges)
    start_all(beside[1::3])
    start_all(beside[2::3])
    arrive_all(row_halo)
    for place in range(2, rows):
        arrive_all(frame_halo[place])
    arrive_all(beside[::3])
    above, below = sides(0)
    for t in own_frames:
        ends(t, above, below)
    (t_first, slot_first), (t_last, slot_last) = beside_frames
    rows_first = rows_in(t_first, dot_t(ub[slot_first, 0], pick))
    rows_last = rows_in(t_last, dot_t(ub[slot_last, 0], pick))
    heavy = [step for t in own_frames for step in products(t, 0, 3)] + products(t_first, 1, 2)
    norms = [functools.partial(second_norm, t) for t in own_frames]
    light = [*rows_first, *(step for n, norm in enumerate(norms) for step in (norm, *rows_last[n : n + 1]))]
    weave(heavy, [*light, *rows_last[len(norms) :]])
    arrive_all(beside[1::3])
    arrive_all(beside[2::3])
    arrive_all(corner_halo)
    weave(
        products(t_last, 1, 2),
        [functools.partial(ends, t, *sides(slot)) for t, slot in beside_frames],
    )
    weave(
        [*products(t_first, 0, 3), *products(t_last, 0, 3), functools.partial(temporal, 0)],
        [lambda: None, lambda: None, functools.partial(second_norm, t_first)],
    )
    second_norm(t_last)
    for t in range(f_dev):
        if t > 0:
            temporal(t)
        finish(t)

    for copies in (gather, scatter, sums, row_halo, *frame_halo, corner_halo, edges, beside):
        sent_all(copies)
    for copy in across:
        copy.wait_send()


def local(fine, coarse, w_qkv, w_out, w_up, gain_one, conv_space, gain_two, conv_time):
    nf = lax.axis_size("frame")
    nr = lax.axis_size("row")
    f_dev, chans, rows, width = fine.shape
    cf_count, p_dev, c_dev = coarse.shape
    cells = cf_count * p_dev
    cc = nf * c_dev
    group = (width // UPSAMPLE) // p_dev
    span = group * p_dev
    any_spec = pl.BlockSpec(memory_space=pl.ANY)
    dma = pltpu.SemaphoreType.DMA
    n_halo = 2 * (1 + 2) + 2 * rows
    out = pl.pallas_call(
        functools.partial(kernel, nf, nr, cf_count, p_dev, rows),
        out_shape=pltpu.VMEM((f_dev, chans * rows, width), BF),
        in_specs=[any_spec] * 9,
        out_specs=pl.BlockSpec(memory_space=pltpu.VMEM),
        scratch_shapes=[
            pltpu.VMEM((cells, c_dev), BF),
            pltpu.VMEM((chans,), F32),
            pltpu.VMEM((chans,), F32),
            pltpu.VMEM((f_dev, chans * rows, width), BF),
            pltpu.VMEM((3, c_dev, cc), BF),
            pltpu.VMEM((c_dev, cc), BF),
            pltpu.VMEM((c_dev, chans), BF),
            pltpu.VMEM((3, 3 * chans, chans), BF),
            pltpu.VMEM((3 * chans, chans), BF),
            pltpu.VMEM((5, pl.cdiv(3 * chans, width), chans, width), BF),
            pltpu.VMEM((f_dev + 2, rows + 2, chans, width), BF),
            pltpu.VMEM((f_dev, rows, chans, width), BF),
            pltpu.VMEM((nf, cells, c_dev), BF),
            pltpu.VMEM((nf, cells, c_dev), BF),
            pltpu.VMEM((nf, cells, c_dev), BF),
            pltpu.VMEM((cf_count, p_dev, chans), BF),
            pltpu.VMEM((group, nf, p_dev, chans), BF),
            pltpu.VMEM((3, 3, span, chans), BF),
            pltpu.VMEM((f_dev + 2, 4, rows // 2, 3 * chans, width), BF),
            pltpu.VMEM((rows, (f_dev + 2) * chans, width), BF),
            pltpu.VMEM((f_dev + 2, 2, chans, width), F32),
            pltpu.VMEM((f_dev + 2, 2, chans, (rows // 2) * width), F32),
            pltpu.VMEM((chans, width), F32),
            pltpu.VMEM((chans, width), F32),
            pltpu.VMEM((f_dev, chans * rows, width), F32),
            dma((11,)),
            dma((n_halo,)),
            dma((n_halo,)),
            dma((2 * nf,)),
            dma((2 * nf,)),
            dma((2 * nf,)),
            dma((2 * nf,)),
            dma((2 * nf, group)),
            dma((2 * nf, group)),
            dma((8,)),
            dma((3, 3)),
        ],
        compiler_params=pltpu.CompilerParams(
            collective_id=0, has_side_effects=True, vmem_limit_bytes=56 * 1024 * 1024
        ),
        name="decoder_window",
    )(
        fine.reshape(f_dev, chans * rows, width),
        coarse.reshape(cells, c_dev),
        jnp.swapaxes(w_qkv, 1, 2),
        w_out,
        w_up,
        gain_one,
        conv_space.reshape(3, 3 * chans, chans),
        gain_two,
        conv_time.reshape(3 * chans, chans),
    )
    return out.reshape(f_dev, chans, rows, width)


def solution(mesh):
    return jax.shard_map(
        local,
        mesh=mesh,
        in_specs=(
            P("frame", None, "row", None),
            P(None, "row", "frame"),
            P(None, None, "frame"),
            P("frame", None),
            P("frame", None),
            P(),
            P(),
            P(),
            P(),
        ),
        out_specs=P("frame", None, "row", None),
        check_vma=False,
    )
```

```python
import functools
import math

import jax
import jax.numpy as jnp
from jax import lax
from jax.experimental import pallas as pl
from jax.experimental.pallas import tpu as pltpu
from jax.sharding import PartitionSpec as P

HD = 80
UPSAMPLE = 8
MESH = pl.DeviceIdType.MESH
BF = jnp.bfloat16
F32 = jnp.float32


def dot(a, b):
    return jnp.dot(a, b, preferred_element_type=F32)


def dot_t(a, b):
    return lax.dot_general(a, b, (((0,), (0,)), ((), ())), preferred_element_type=F32)


def norm_silu(v, half_gain):
    scale = lax.rsqrt(jnp.mean(v * v, axis=0, keepdims=True) + 1e-06)
    half = v * scale * half_gain
    return half + half * jnp.tanh(half)


def kernel(
    nf, nr, cf_count, p_dev, rows,
    fine_ref, coarse_ref, w_qkv_ref, w_out_ref, w_up_ref, gain_one_ref, conv_s_ref, gain_two_ref, conv_t_ref,
    out_ref,
    cv, g1, g2, ff, wq, wo, wu, cs, ct, wt, fb, mg, cg, rs_send, rs_recv, up_send, up_recv, ub, x3, n2, keep, acc,
    half_one, half_two, o32,
    load_sem, halo_send, halo_recv, g_send, g_recv, r_send, r_recv, u_send, u_recv, b_send, b_recv,
):
    f_dev, flat, width = fine_ref.shape
    chans = flat // rows
    cells, c_dev = coarse_ref.shape
    frames_ext = f_dev + 2
    rows_ext = rows + 2
    group = (width // UPSAMPLE) // p_dev
    n_groups = nr // group
    heads = c_dev // HD
    span = group * p_dev
    total_frames = nf * f_dev
    me_f = lax.axis_index("frame")
    me_r = lax.axis_index("row")
    my_group = me_r // group
    k_me = me_r % group
    base = my_group * group
    first = k_me == 0
    last = k_me == group - 1
    has_above = first & (my_group > 0)
    has_below = last & (my_group < n_groups - 1)

    def dev(f, r):
        return {"frame": f, "row": r}

    barrier = pltpu.get_barrier_semaphore()
    for step_f in range(nf):
        for step_k in range(group):
            if step_f or step_k:
                peer = dev((me_f + step_f) % nf, base + (k_me + step_k) % group)
                pl.semaphore_signal(barrier, inc=1, device_id=peer, device_id_type=MESH)
    expected = jnp.int32(nf * group - 1)
    for ok, peer in ((has_above, me_r - 1), (has_below, me_r + 1)):
        expected = expected + ok.astype(jnp.int32)

        @pl.when(ok)
        def _(peer=peer):
            pl.semaphore_signal(barrier, inc=1, device_id=dev(me_f, peer), device_id_type=MESH)

    parts = {
        "coarse": (coarse_ref, cv),
        "fine": (fine_ref, ff),
        "gain_one": (gain_one_ref, g1),
        "gain_two": (gain_two_ref, g2),
        "qkv": (w_qkv_ref, wq),
        "out": (w_out_ref, wo),
        "space0": (conv_s_ref.at[0], cs.at[0]),
        "up": (w_up_ref, wu),
        "space1": (conv_s_ref.at[1], cs.at[1]),
        "space2": (conv_s_ref.at[2], cs.at[2]),
        "time": (conv_t_ref, ct),
    }
    loads = {
        name: pltpu.make_async_copy(src, dst, load_sem.at[n])
        for n, (name, (src, dst)) in enumerate(parts.items())
    }
    for load in loads.values():
        load.start()

    def start_all(copies):
        for copy, there, _ in copies:

            @pl.when(there)
            def _(copy=copy):
                copy.start()

    def arrive_all(copies):
        for copy, _, source in copies:

            @pl.when(source)
            def _(copy=copy):
                copy.wait_recv()

    def sent_all(copies):
        for copy, there, _ in copies:

            @pl.when(there)
            def _(copy=copy):
                copy.wait_send()

    def over_frames(make):
        copies = []
        for n, (far, d) in enumerate((far, d) for far in range(nf - 1, 0, -1) for d in (-1, 1)):
            there = (me_f + d * far >= 0) & (me_f + d * far < nf)
            source = (me_f - d * far >= 0) & (me_f - d * far < nf)
            copies.append((make(n, (me_f + d * far + nf) % nf), there, source))
        return copies

    gather = over_frames(
        lambda n, peer: pltpu.make_async_remote_copy(
            src_ref=cv,
            dst_ref=cg.at[me_f],
            send_sem=g_send.at[n],
            recv_sem=g_recv.at[n],
            device_id=dev(peer, me_r),
            device_id_type=MESH,
        )
    )
    loads["coarse"].wait()
    pl.semaphore_wait(barrier, expected)
    start_all(gather)
    cg[me_f] = cv[...]

    loads["fine"].wait()
    block = math.gcd(chans, 64)
    size = block * rows
    i = lax.broadcasted_iota(jnp.int32, (size, size), 0)
    k = lax.broadcasted_iota(jnp.int32, (size, size), 1)
    sort_rows = jnp.where((k % rows == i // block) & (k // rows == i % block), 1.0, 0.0).astype(BF)
    for b in range(chans // block):
        mixed_rows = jnp.concatenate([ff[t, b * size : (b + 1) * size, :] for t in range(f_dev)], axis=1)
        sorted_rows = dot(sort_rows, mixed_rows).astype(BF)
        for t in range(f_dev):
            for r in range(rows):
                fb[1 + t, 1 + r, b * block : (b + 1) * block, :] = sorted_rows[
                    r * block : (r + 1) * block, t * width : (t + 1) * width
                ]

    def remote(n, src, dst, f, r):
        return pltpu.make_async_remote_copy(
            src_ref=src,
            dst_ref=dst,
            send_sem=halo_send.at[n],
            recv_sem=halo_recv.at[n],
            device_id=dev(f, r),
            device_id_type=MESH,
        )

    own_f = pl.ds(1, f_dev)
    row_order = [0, rows - 1, *range(1, rows - 1)] if rows > 1 else [0]
    row_halo, corner_halo = [], []
    frame_halo = [[] for _ in row_order]
    at_frame = ((0, me_f > 0), (frames_ext - 1, me_f < nf - 1))
    n_sem = 0
    for d in (-1, 1):
        there = (me_r + d >= 0) & (me_r + d < nr)
        source = (me_r - d >= 0) & (me_r - d < nr)
        src_r, dst_r = (rows, 0) if d > 0 else (1, rows_ext - 1)
        row_halo.append(
            (remote(n_sem, fb.at[own_f, src_r], fb.at[own_f, dst_r], me_f, me_r + d), there, source)
        )
        n_sem += 1
        for at, exists in at_frame:
            corner_halo.append(
                (remote(n_sem, fb.at[at, src_r], fb.at[at, dst_r], me_f, me_r + d), there & exists, source & exists)
            )
            n_sem += 1
    for d in (-1, 1):
        there = (me_f + d >= 0) & (me_f + d < nf)
        source = (me_f - d >= 0) & (me_f - d < nf)
        src_f, dst_f = (f_dev, 0) if d > 0 else (1, frames_ext - 1)
        for place, r in enumerate(row_order):
            copy = remote(n_sem, fb.at[src_f, 1 + r], fb.at[dst_f, 1 + r], me_f + d, me_r)
            frame_halo[place].append((copy, there, source))
            n_sem += 1

    start_all(frame_halo[0])

    for edge, at in ((me_r == 0, 0), (me_r == nr - 1, rows_ext - 1)):

        @pl.when(edge)
        def _(at=at):
            fb[:, at] = jnp.zeros((frames_ext, chans, width), BF)

    for edge, at in ((me_f == 0, 0), (me_f == nf - 1, frames_ext - 1)):

        @pl.when(edge)
        def _(at=at):
            fb[at] = jnp.zeros((rows_ext, chans, width), BF)

    for edge, region in ((first & (my_group == 0), 1), (last & (my_group == n_groups - 1), 2)):

        @pl.when(edge)
        def _(region=region):
            ub[:, region] = jnp.zeros((3, span, chans), BF)

    for edge, slot in ((me_f == 0, 1), (me_f == nf - 1, 2)):

        @pl.when(edge)
        def _(slot=slot):
            ub[slot] = jnp.zeros((3, span, chans), BF)

    loads["gain_one"].wait()
    loads["gain_two"].wait()
    half_one[...] = jnp.broadcast_to(0.5 * g1[...][None, :], (width, chans)).T
    half_two[...] = jnp.broadcast_to(0.5 * g2[...][None, :], (width, chans)).T

    pieces = [(start, min(width, 3 * chans - start)) for start in range(0, 3 * chans, width)]

    def lay(n, weights):
        for piece, (start, size) in enumerate(pieces):
            wt[n, piece, :, 0:size] = weights[start : start + size].T

    def wide(ref, n):
        return jnp.concatenate([ref[n, piece, :, 0:size] for piece, (_, size) in enumerate(pieces)], axis=1)

    loads["qkv"].wait()
    loads["space0"].wait()
    lay(0, cs[0])
    arrive_all(gather)
    cells_all = jnp.concatenate([cg[j].astype(F32) for j in range(nf)], axis=1).astype(BF)
    qkv = []
    for i in range(3):
        product = lax.dot_general(
            cells_all, wq[i], (((1,), (1,)), ((), ())), preferred_element_type=F32
        )
        qkv.append(product.astype(BF))
    query, keys, values = qkv

    head_of_lane = lax.broadcasted_iota(jnp.int32, (cells, c_dev), 1) // HD
    spread = jnp.concatenate(
        [jnp.where(head_of_lane == h, query.astype(F32), 0.0) for h in range(heads)], axis=0
    ).astype(BF)
    scores = lax.dot_general(
        spread, keys, (((1,), (1,)), ((), ())), preferred_element_type=F32
    ) / math.sqrt(HD)
    cell_q = lax.broadcasted_iota(jnp.int32, scores.shape, 0) % p_dev
    cell_k = lax.broadcasted_iota(jnp.int32, scores.shape, 1) % p_dev
    same = cell_q == cell_k
    scores = jnp.where(same, scores, -1e30)
    top = jnp.max(scores, axis=1, keepdims=True)
    weight = jnp.where(same, jnp.exp(scores - top), 0.0)
    probs = (weight / jnp.sum(weight, axis=1, keepdims=True)).astype(BF)
    mixed = dot(probs, values)
    attn = None
    for h in range(heads):
        part = jnp.where(head_of_lane == h, mixed[h * cells : (h + 1) * cells], 0.0)
        attn = part if attn is None else attn + part
    attn = attn.astype(BF)

    loads["out"].wait()
    partial_out = dot(attn, wo[...])
    for j in range(nf):
        rs_send[j] = partial_out[:, j * c_dev : (j + 1) * c_dev].astype(BF)

    scatter = over_frames(
        lambda n, peer: pltpu.make_async_remote_copy(
            src_ref=rs_send.at[peer],
            dst_ref=rs_recv.at[me_f],
            send_sem=r_send.at[n],
            recv_sem=r_recv.at[n],
            device_id=dev(peer, me_r),
            device_id_type=MESH,
        )
    )
    start_all(scatter)
    start_all(row_halo)
    if rows > 1:
        start_all(frame_halo[1])
    rs_recv[me_f] = rs_send[me_f]
    loads["space1"].wait()
    loads["space2"].wait()
    lay(1, ((cs[0].astype(F32) + cs[2].astype(F32) + cs[1].astype(F32)) * 0.5).astype(BF))
    lay(3, cs[2])
    loads["up"].wait()
    arrive_all(scatter)
    share = cv[...].astype(F32)
    for j in range(nf):
        share = share + rs_recv[j].astype(F32)
    up_partial = dot(share.astype(BF), wu[...])
    for j in range(cf_count):
        up_send[j] = up_partial[j * p_dev : (j + 1) * p_dev].astype(BF)

    def coarse_frame(f):
        return (f * f_dev * cf_count) // total_frames

    def sum_copy(n, step_k, peer):
        return pltpu.make_async_remote_copy(
            src_ref=up_send.at[coarse_frame(peer)],
            dst_ref=up_recv.at[k_me, me_f],
            send_sem=u_send.at[n, step_k],
            recv_sem=u_recv.at[n, step_k],
            device_id=dev(peer, base + (k_me + step_k) % group),
            device_id_type=MESH,
        )

    sums = [copy for step_k in range(group) for copy in over_frames(lambda n, peer: sum_copy(n, step_k, peer))]
    sums = [sums[n + step_k * len(scatter)] for n in range(len(scatter)) for step_k in range(group)]
    for copy in sums:
        start_all([copy])
    across = [sum_copy(len(scatter), step_k, me_f) for step_k in range(1, group)]
    for copy in across:
        copy.start()
    up_recv[k_me, me_f] = up_send[coarse_frame(me_f)]
    for place in range(2, rows):
        start_all(frame_halo[place])
    lay(2, ((cs[0].astype(F32) + cs[2].astype(F32) - cs[1].astype(F32)) * 0.5).astype(BF))
    loads["time"].wait()
    lay(4, ct[...])
    rho = lax.broadcasted_iota(jnp.int32, (span, width), 0)
    lane = lax.broadcasted_iota(jnp.int32, (span, width), 1)
    pick = jnp.where(lane // UPSAMPLE == rho, 1.0, 0.0).astype(BF)
    arrive_all(sums)
    for copy in across:
        copy.wait_recv()
    halves = []
    for c in range(group):
        up = up_recv[c, 0].astype(F32)
        for j in range(1, nf):
            up = up + up_recv[c, j].astype(F32)
        halves.append(up)
    ub[0, 0] = (jnp.concatenate(halves, axis=0) if group > 1 else halves[0]).astype(BF)

    def block_copy(n, src, slot, region, f, r):
        return pltpu.make_async_remote_copy(
            src_ref=ub.at[0, src],
            dst_ref=ub.at[slot, region],
            send_sem=b_send.at[n],
            recv_sem=b_recv.at[slot, region],
            device_id=dev(f, r),
            device_id_type=MESH,
        )

    edges = [
        (block_copy(0, 0, 0, 1, me_f, me_r + 1), has_below, has_above),
        (block_copy(1, 0, 0, 2, me_f, me_r - 1), has_above, has_below),
    ]
    beside = []
    n_block = 2
    for slot, d in ((1, 1), (2, -1)):
        there = (me_f + d >= 0) & (me_f + d < nf)
        source = (me_f - d >= 0) & (me_f - d < nf)
        for region, have in ((0, None), (1, has_above), (2, has_below)):
            copy = block_copy(n_block, region, slot, region, me_f + d, me_r)
            n_block += 1
            beside.append((copy, there, source) if have is None else (copy, there & have, source & have))
    start_all(edges)
    start_all(beside[::3])
    arrive_all(frame_halo[0])
    if rows > 1:
        arrive_all(frame_halo[1])
    start_all(corner_halo)

    lane_bf = lax.broadcasted_iota(jnp.int32, (chans, width), 1)
    keep_left = jnp.where(lane_bf == 0, 0.0, 1.0).astype(BF)
    keep_right = jnp.where(lane_bf == width - 1, 0.0, 1.0).astype(BF)

    tiles = rows // 2

    def activate(t, r, widened):
        v = fb[t, r].astype(F32) + widened
        if 0 < t < frames_ext - 1 and 0 < r < rows_ext - 1:
            mg[t - 1, r - 1] = v.astype(BF)
        return norm_silu(v, half_one[...])

    def put(t, n, tile, v):
        v = v.astype(BF)
        x3[t, n, tile, chans : 2 * chans] = v
        x3[t, n, tile, 0:chans] = pltpu.roll(v, 1, 1) * keep_left
        x3[t, n, tile, 2 * chans : 3 * chans] = pltpu.roll(v, width - 1, 1) * keep_right

    def product(t, n):
        return dot(wide(wt, n), jnp.concatenate([x3[t, n, tile] for tile in range(tiles)], axis=1))

    act, term = {}, {}

    def rows_in(t, widened):
        def one(tile):
            r = 2 * tile + 1
            act[t, r] = activate(t, r, widened)
            act[t, r + 1] = activate(t, r + 1, widened)
            put(t, 1, tile, act[t, r] + act[t, r + 1])
            put(t, 2, tile, act[t, r + 1] - act[t, r])
            if tile > 0:
                put(t, 0, tile, act[t, r - 1] - act[t, r + 1])
                put(t, 3, tile - 1, act[t, r - 2] - act[t, r])
            if r + 1 == 2:
                keep[t, 0] = act[t, 2]
            if tile == tiles - 1:
                keep[t, 1] = act[t, rows - 1]

        return [functools.partial(one, tile) for tile in range(tiles)]

    def multiply(t, n):
        term[t, n] = product(t, n)
        if n == 2:
            acc[t, 0] = term[t, 1] + term[t, 2]
            acc[t, 1] = term[t, 1] - term[t, 2]

    def products(t, *which):
        return [functools.partial(multiply, t, n) for n in which]

    def ends(t, above, below):
        put(t, 0, 0, activate(t, 0, above) - keep[t, 0])
        put(t, 3, tiles - 1, keep[t, 1] - activate(t, rows_ext - 1, below))

    def second_norm(t):
        pair = (acc[t, 0] + term[t, 0], acc[t, 1] - term[t, 3])
        for r in range(rows):
            from_tile = slice((r // 2) * width, (r // 2 + 1) * width)
            n2[r, t * chans : (t + 1) * chans] = norm_silu(pair[r % 2][:, from_tile], half_two[...]).astype(BF)

    def temporal(t):
        window = jnp.concatenate([n2[r, t * chans : (t + 3) * chans] for r in range(rows)], axis=1)
        term[t] = dot(wide(wt, 4), window)

    def finish(t):
        for r in range(rows):
            here = slice(r * width, (r + 1) * width)
            o32[t, pl.ds(r, chans, rows), :] = mg[t, r].astype(F32) + term[t][:, here]
        out_ref[t] = o32[t].astype(BF)

    def weave(first_list, second_list):
        for n in range(max(len(first_list), len(second_list))):
            for steps in (first_list, second_list):
                if n < len(steps):
                    steps[n]()

    def sides(slot):
        return (
            dot_t(ub[slot, jnp.where(first, 1, 0)], pick),
            dot_t(ub[slot, jnp.where(last, 2, 0)], pick),
        )

    beside_frames = ((0, 1), (frames_ext - 1, 2))
    own = dot_t(ub[0, 0], pick)
    own_frames = range(1, frames_ext - 1)
    before = []
    for t in own_frames:
        weave(before, rows_in(t, own))
        before = products(t, 1, 2)
    weave(before, [])
    arrive_all(edges)
    start_all(beside[1::3])
    start_all(beside[2::3])
    arrive_all(row_halo)
    for place in range(2, rows):
        arrive_all(frame_halo[place])
    arrive_all(beside[::3])
    above, below = sides(0)
    for t in own_frames:
        ends(t, above, below)
    (t_first, slot_first), (t_last, slot_last) = beside_frames
    rows_first = rows_in(t_first, dot_t(ub[slot_first, 0], pick))
    rows_last = rows_in(t_last, dot_t(ub[slot_last, 0], pick))
    heavy = [step for t in own_frames for step in products(t, 0, 3)] + products(t_first, 1, 2)
    norms = [functools.partial(second_norm, t) for t in own_frames]
    light = [*rows_first, *(step for n, norm in enumerate(norms) for step in (norm, *rows_last[n : n + 1]))]
    weave(heavy, [*light, *rows_last[len(norms) :]])
    arrive_all(beside[1::3])
    arrive_all(beside[2::3])
    arrive_all(corner_halo)
    weave(
        products(t_last, 1, 2),
        [functools.partial(ends, t, *sides(slot)) for t, slot in beside_frames],
    )
    weave(
        [*products(t_first, 0, 3), *products(t_last, 0, 3), functools.partial(temporal, 0)],
        [lambda: None, lambda: None, functools.partial(second_norm, t_first)],
    )
    second_norm(t_last)
    for t in range(f_dev):
        if t > 0:
            temporal(t)
        finish(t)

    for copies in (gather, scatter, sums, row_halo, *frame_halo, corner_halo, edges, beside):
        sent_all(copies)
    for copy in across:
        copy.wait_send()


def local(fine, coarse, w_qkv, w_out, w_up, gain_one, conv_space, gain_two, conv_time):
    nf = lax.axis_size("frame")
    nr = lax.axis_size("row")
    f_dev, chans, rows, width = fine.shape
    cf_count, p_dev, c_dev = coarse.shape
    cells = cf_count * p_dev
    cc = nf * c_dev
    group = (width // UPSAMPLE) // p_dev
    span = group * p_dev
    any_spec = pl.BlockSpec(memory_space=pl.ANY)
    dma = pltpu.SemaphoreType.DMA
    n_halo = 2 * (1 + 2) + 2 * rows
    out = pl.pallas_call(
        functools.partial(kernel, nf, nr, cf_count, p_dev, rows),
        out_shape=pltpu.VMEM((f_dev, chans * rows, width), BF),
        in_specs=[any_spec] * 9,
        out_specs=pl.BlockSpec(memory_space=pltpu.VMEM),
        scratch_shapes=[
            pltpu.VMEM((cells, c_dev), BF),
            pltpu.VMEM((chans,), F32),
            pltpu.VMEM((chans,), F32),
            pltpu.VMEM((f_dev, chans * rows, width), BF),
            pltpu.VMEM((3, c_dev, cc), BF),
            pltpu.VMEM((c_dev, cc), BF),
            pltpu.VMEM((c_dev, chans), BF),
            pltpu.VMEM((3, 3 * chans, chans), BF),
            pltpu.VMEM((3 * chans, chans), BF),
            pltpu.VMEM((5, pl.cdiv(3 * chans, width), chans, width), BF),
            pltpu.VMEM((f_dev + 2, rows + 2, chans, width), BF),
            pltpu.VMEM((f_dev, rows, chans, width), BF),
            pltpu.VMEM((nf, cells, c_dev), BF),
            pltpu.VMEM((nf, cells, c_dev), BF),
            pltpu.VMEM((nf, cells, c_dev), BF),
            pltpu.VMEM((cf_count, p_dev, chans), BF),
            pltpu.VMEM((group, nf, p_dev, chans), BF),
            pltpu.VMEM((3, 3, span, chans), BF),
            pltpu.VMEM((f_dev + 2, 4, rows // 2, 3 * chans, width), BF),
            pltpu.VMEM((rows, (f_dev + 2) * chans, width), BF),
            pltpu.VMEM((f_dev + 2, 2, chans, width), F32),
            pltpu.VMEM((f_dev + 2, 2, chans, (rows // 2) * width), F32),
            pltpu.VMEM((chans, width), F32),
            pltpu.VMEM((chans, width), F32),
            pltpu.VMEM((f_dev, chans * rows, width), F32),
            dma((11,)),
            dma((n_halo,)),
            dma((n_halo,)),
            dma((2 * nf,)),
            dma((2 * nf,)),
            dma((2 * nf,)),
            dma((2 * nf,)),
            dma((2 * nf, group)),
            dma((2 * nf, group)),
            dma((8,)),
            dma((3, 3)),
        ],
        compiler_params=pltpu.CompilerParams(
            collective_id=0, has_side_effects=True, vmem_limit_bytes=56 * 1024 * 1024
        ),
        name="decoder_window",
    )(
        fine.reshape(f_dev, chans * rows, width),
        coarse.reshape(cells, c_dev),
        jnp.swapaxes(w_qkv, 1, 2),
        w_out,
        w_up,
        gain_one,
        conv_space.reshape(3, 3 * chans, chans),
        gain_two,
        conv_time.reshape(3 * chans, chans),
    )
    return out.reshape(f_dev, chans, rows, width)


def solution(mesh):
    return jax.shard_map(
        local,
        mesh=mesh,
        in_specs=(
            P("frame", None, "row", None),
            P(None, "row", "frame"),
            P(None, None, "frame"),
            P("frame", None),
            P("frame", None),
            P(),
            P(),
            P(),
            P(),
        ),
        out_specs=P("frame", None, "row", None),
        check_vma=False,
    )
```
